32 devices in a mesh: batch: 8 (over z, x), head: 4 (over y, core).
Axes of the slice: x: 2, y: 2, z: 4, core: 2. Of those that a mesh axis runs over, the one named last changes fastest.
Arguments:
- tokens: bfloat16 [4096, 2048], P('batch', 'head'), may hold values from -96 to 96
- lengths: int32 [32], P('batch'), may hold values from 1 to 128
- states: float32 [32, 16, 128, 128], P('batch', 'head'), may hold values from -3 to 3
- norm_gain: float32 [2048], replicated, may hold values from 0.1 to 1.9
- mix_weight: bfloat16 [2048, 14336], P(None, 'head'), may hold values from -0.125 to 0.125
- rate_weight: bfloat16 [2048, 64], P(None, 'head'), may hold values from -0.5524272 to 0.5524272
- decay_rate: float32 [16], P('head'), may hold values from 0.0005 to 0.03
- head_gain: float32 [128], replicated, may hold values from 0.1 to 1.9
- out_weight: bfloat16 [2048, 2048], P('head'), may hold values from -0.125 to 0.125
- final_gain: float32 [2048], replicated, may hold values from 0.1 to 1.9
- vocab_table: bfloat16 [16384, 2048], P(('batch', 'head')), may hold values from -50.8233 to 50.8233
- next_token: int32 [32], replicated, may hold values from 0 to 16383
Outputs:
- mixed: bfloat16 [4096, 2048], P('batch', 'head')
- new_state: float32 [32, 16, 128, 128], P('batch', 'head')
- log_likelihood: float32 [32], replicated
The draws below stay inside these ranges and needn't reach their ends.
All inputs are finite; a program needn't handle non-finite values.
Results may differ from the reference program's by a relative error of at most 0.0058.
The reference program's roundings to bfloat16 on the way count: a program that leaves them out, or rounds other values in their place, can miss the bound.
Values may be sent and summed in bfloat16 or wider, within the bound.
No kernel may reach another device: no remote copies, remote signals or barrier semaphores. Data moves between devices by JAX's collectives and lax.ppermute only.
A program may use at most 128 MiB of HBM per device.

```python
import math
import jax
import jax.numpy as jnp
import numpy as np
from jax import lax

D = 2048
HEADS = 16
HEAD_DIM = 128
REFLECT = 3
VOCAB = 16384
NEW_POSITIONS = 128
SEQUENCE_COUNT = 32
TOKEN_ROWS_ALL = 4096


def householder_directions(key):
    reflect_vectors = jnp.clip(jax.random.normal(jax.random.fold_in(key, 101), (D, HEADS), jnp.float32), -4.0, 4.0)
    return reflect_vectors / jnp.sqrt(1.0 * D)


def draw_tokens(key, part):
    reflect_vectors = householder_directions(key)
    shared_way = jnp.sum(reflect_vectors, axis=1)
    shared_way = shared_way / jnp.sqrt(jnp.sum(shared_way * shared_way))
    column_scale = 0.3 * 10.0 ** (jnp.arange(D, dtype=jnp.float32) / (D - 1))
    row_scale = 10.0 ** jax.random.uniform(jax.random.fold_in(key, 102), (TOKEN_ROWS_ALL, 1), jnp.float32, -1.0, 0.0)
    base = jnp.clip(jax.random.normal(jax.random.fold_in(key, 103), (TOKEN_ROWS_ALL, D), jnp.float32), -4.0, 4.0)
    values = base * row_scale * column_scale
    householder_steps = jax.random.randint(jax.random.fold_in(key, 105), (SEQUENCE_COUNT, 2), 0, NEW_POSITIONS)
    position_places = jnp.arange(NEW_POSITIONS)
    masked_entries = jnp.any(position_places[None, :, None] == householder_steps[:, None, :], axis=2).reshape(TOKEN_ROWS_ALL, 1)
    values = values + jnp.where(masked_entries, 80.0 * shared_way[None, :], 0.0)
    return values.astype(jnp.bfloat16)


def draw_rate_weight(key, part):
    reflect_vectors = householder_directions(key)
    noise = jnp.clip(jax.random.normal(jax.random.fold_in(key, 111), (D, HEADS, REFLECT + 1), jnp.float32), -5.0, 5.0)
    noise = noise / jnp.sqrt(1.0 * D)
    boost = jnp.concatenate([jnp.zeros((D, HEADS, REFLECT), jnp.float32), 5.0 * reflect_vectors[:, :, None]], axis=2)
    return (noise + boost).reshape(D, HEADS * (REFLECT + 1)).astype(jnp.bfloat16)


def draw_decay_rate(key, part):
    spread = jax.random.uniform(jax.random.fold_in(key, 121), (HEADS,), jnp.float32)
    rates = 0.002 * 15.0 ** spread
    return rates


def draw_vocab_table(key, part):
    row_scale = 10.0 ** jax.random.uniform(jax.random.fold_in(key, 131), (VOCAB, 1), jnp.float32)
    base = jnp.clip(jax.random.normal(jax.random.fold_in(key, 132), (VOCAB, D), jnp.float32), -5.0, 5.0)
    values = base * row_scale / jnp.sqrt(1.0 * D)
    return values.astype(jnp.bfloat16)


def touch_ends(values, own_key, least, high):
    extent = values.shape
    index_at = [jax.random.randint(jax.random.fold_in(own_key, axis), (), 0, extent[axis]) for axis in range(len(extent))]
    values = values.at[tuple(index_at)].set(least)
    longest = extent.index(max(extent))
    index_at[longest] = (index_at[longest] + 1) % extent[longest]
    return values.at[tuple(index_at)].set(high)


def level_of(own_key, dims, split, smallest, top_value):
    gain, own = 1.0, jax.random.fold_in(own_key, 6)
    for axis_at, blocks in split:
        heights = jnp.exp(jax.random.uniform(jax.random.fold_in(own, axis_at), (blocks,), jnp.float32, smallest / len(split), top_value / len(split)))
        gain = gain * jnp.repeat(heights, dims[axis_at] // blocks).reshape([-1 if axis == axis_at else 1 for axis in range(len(dims))])
    return gain


def rank_bounds(amount, slope):
    loads = [(1 << 20) // math.isqrt(rank ** slope) + 1 for rank in range(1, amount + 1)]
    scale = 1 + sum(loads) // (1 << 30)
    return np.cumsum(np.array([max(1, weight // scale) for weight in loads]))


def ranked(key, shape, number_of, slope):
    table = rank_bounds(number_of, slope)
    ticket = jax.random.randint(jax.random.fold_in(key, 1), shape, 0, int(table[number_of - 1]))
    standing = jnp.searchsorted(jnp.asarray(table, jnp.int32), ticket, side="right")
    return jax.random.permutation(jax.random.fold_in(key, 2), number_of)[standing].astype(jnp.int32)


def bell_draw(stream_key, shape, scale, most, cuts=(), kind=jnp.bfloat16):
    drawn = jax.random.normal(stream_key, shape, jnp.float32) * scale
    if len(cuts) > 0:
        drawn = level_of(stream_key, shape, cuts, -0.22, 0.18) * drawn
    return jnp.clip(drawn, min=-most, max=most).astype(kind)


def setup_inputs(seed: int = 0) -> dict:
    streams_of = jax.random.split(jax.random.key(seed), 13)
    tokens = draw_tokens(jax.random.fold_in(streams_of[12], 71), 0)
    lengths = touch_ends(jax.random.randint(streams_of[1], (SEQUENCE_COUNT,), 1, NEW_POSITIONS + 1), jax.random.fold_in(streams_of[1], 1), 1, NEW_POSITIONS).astype(jnp.int32)
    states = bell_draw(streams_of[2], (SEQUENCE_COUNT, HEADS, HEAD_DIM, HEAD_DIM), 0.5, 3.0, ((0, 8), (1, 4)), jnp.float32)
    norm_gain = jnp.clip(1.0 + 0.18 * jax.random.normal(streams_of[3], (D,), jnp.float32), 0.1, 1.9)
    mix_weight = bell_draw(streams_of[4], (D, HEADS * (2 * REFLECT + 1) * HEAD_DIM), D ** -0.5, 0.125, ((1, 4),))
    rate_weight = draw_rate_weight(jax.random.fold_in(streams_of[12], 71), 0)
    decay_rate = draw_decay_rate(jax.random.fold_in(streams_of[12], 71), 0)
    head_gain = jnp.clip(1.0 + 0.18 * jax.random.normal(streams_of[7], (HEAD_DIM,), jnp.float32), 0.1, 1.9)
    out_weight = bell_draw(streams_of[8], (HEADS * HEAD_DIM, D), (HEADS * HEAD_DIM) ** -0.5, 0.125, ((0, 4),))
    final_gain = jnp.clip(1.0 + 0.18 * jax.random.normal(streams_of[9], (D,), jnp.float32), 0.1, 1.9)
    vocab_table = draw_vocab_table(jax.random.fold_in(streams_of[12], 71), 0)
    next_token = touch_ends(ranked(streams_of[11], (SEQUENCE_COUNT,), VOCAB, 2), jax.random.fold_in(streams_of[11], 3), 0, VOCAB - 1).astype(jnp.int32)
    return dict(tokens=tokens, lengths=lengths, states=states, norm_gain=norm_gain, mix_weight=mix_weight, rate_weight=rate_weight, decay_rate=decay_rate, head_gain=head_gain, out_weight=out_weight, final_gain=final_gain, vocab_table=vocab_table, next_token=next_token)


ROW_EPSILON = 1e-05
KEY_EPSILON = 1e-06
HIGHEST_PRECISION = lax.Precision.HIGHEST

def delta_block(queries, key_rows, value_rows, beta_rows, log_decay, start_state):
    positions = key_rows.shape[0]
    reflections = key_rows.shape[1]
    total_steps = positions * reflections
    flat_keys = key_rows.reshape(total_steps, key_rows.shape[2])
    flat_values = value_rows.reshape(total_steps, value_rows.shape[2])
    flat_betas = beta_rows.reshape(total_steps)
    padding = jnp.zeros((positions, reflections - 1), log_decay.dtype)
    step_decay = jnp.concatenate([log_decay[:, None], padding], axis=1).reshape(total_steps)
    cumulative = jnp.cumsum(step_decay)
    step_index = jnp.arange(total_steps)
    earlier = step_index[:, None] > step_index[None, :]
    decay_ratio = jnp.exp(jnp.where(earlier, cumulative[:, None] - cumulative[None, :], -jnp.inf))
    key_gram = jnp.dot(flat_keys, flat_keys.T, precision=HIGHEST_PRECISION)
    system = jnp.eye(total_steps, dtype=key_gram.dtype) + flat_betas[:, None] * decay_ratio * key_gram
    start_image = jnp.dot(flat_keys, start_state.T, precision=HIGHEST_PRECISION)
    source = flat_betas[:, None] * (flat_values - jnp.exp(cumulative)[:, None] * start_image)
    updates = jax.scipy.linalg.solve_triangular(system, source, lower=True, unit_diagonal=True)
    query_cumulative = cumulative.reshape(positions, reflections)[:, reflections - 1]
    query_step = step_index.reshape(positions, reflections)[:, reflections - 1]
    visible = step_index[None, :] <= query_step[:, None]
    weights = jnp.exp(jnp.where(visible, query_cumulative[:, None] - cumulative[None, :], -jnp.inf))
    scores = jnp.dot(queries, flat_keys.T, precision=HIGHEST_PRECISION) * weights
    attended = jnp.exp(query_cumulative)[:, None] * jnp.dot(queries, start_state.T, precision=HIGHEST_PRECISION)
    attended = attended + jnp.dot(scores, updates, precision=HIGHEST_PRECISION)
    tail_decay = jnp.exp(cumulative[total_steps - 1] - cumulative)
    new_state = jnp.exp(cumulative[total_steps - 1]) * start_state
    new_state = new_state + jnp.dot(updates.T, tail_decay[:, None] * flat_keys, precision=HIGHEST_PRECISION)
    return (attended, new_state)

def head_inputs(projected, rate_logits, valid_mask, decay_rate):
    queries = jax.nn.silu(projected[:, :, :, 0])
    key_rows = jax.nn.silu(projected[:, :, :, 1:REFLECT + 1])
    key_rows = key_rows * lax.rsqrt(lax.optimization_barrier(jnp.sum(key_rows * key_rows, axis=-1, keepdims=True)) + KEY_EPSILON)
    value_rows = jax.nn.silu(projected[:, :, :, REFLECT + 1:])
    beta_rows = jnp.where(valid_mask[:, :, None, None], 2.0 * jax.nn.sigmoid(rate_logits[..., :REFLECT]), 0.0)
    log_decay = jnp.where(valid_mask[:, :, None], -decay_rate * jax.nn.softplus(rate_logits[..., REFLECT]), 0.0)
    return (queries, key_rows, value_rows, beta_rows, log_decay)

def run_heads(queries, key_rows, value_rows, beta_rows, log_decay, start_states):
    per_head = jax.vmap(delta_block, in_axes=(1, 1, 1, 1, 1, 0), out_axes=(1, 0))
    per_sequence = jax.vmap(per_head)
    return per_sequence(queries, key_rows, value_rows, beta_rows, log_decay, start_states)

def head_norm(attended, head_gain):
    factor = lax.rsqrt(lax.optimization_barrier(jnp.mean(attended * attended, axis=-1, keepdims=True)) + ROW_EPSILON)
    return (attended * factor * head_gain).astype(jnp.bfloat16)

def reference(tokens, lengths, states, norm_gain, mix_weight, rate_weight, decay_rate, head_gain, out_weight, final_gain, vocab_table, next_token):
    model_width = tokens.shape[1]
    blocks = tokens.reshape(lengths.shape[0], NEW_POSITIONS, model_width)

    def one_sequence(inputs):
        block_rows, length, start_state = inputs
        widened = block_rows.astype(jnp.float32)
        scaled = (widened * norm_gain).astype(jnp.bfloat16)
        inverse = lax.rsqrt(lax.optimization_barrier(jnp.mean(widened * widened, axis=1, keepdims=True)) + ROW_EPSILON)
        projected = jnp.dot(scaled.astype(jnp.float32), mix_weight.astype(jnp.float32), preferred_element_type=jnp.float32) * inverse
        rate_logits = jnp.dot(scaled.astype(jnp.float32), rate_weight.astype(jnp.float32), preferred_element_type=jnp.float32) * inverse
        projected = projected.reshape(1, NEW_POSITIONS, HEADS, 2 * REFLECT + 1, HEAD_DIM)
        rate_logits = rate_logits.reshape(1, NEW_POSITIONS, HEADS, REFLECT + 1)
        valid_mask = (jnp.arange(NEW_POSITIONS) < length)[None, :]
        queries, key_rows, value_rows, beta_rows, log_decay = head_inputs(projected, rate_logits, valid_mask, decay_rate)
        attended, new_state = run_heads(queries, key_rows, value_rows, beta_rows, log_decay, start_state[None])
        normed = head_norm(attended, head_gain).reshape(NEW_POSITIONS, HEADS * HEAD_DIM)
        mixed = (widened + jnp.dot(normed.astype(jnp.float32), out_weight.astype(jnp.float32), preferred_element_type=jnp.float32)).astype(jnp.bfloat16)
        last_row = lax.dynamic_slice_in_dim(mixed, (length - 1).astype(jnp.int32), 1, 0)[0]
        return (mixed, new_state[0], last_row)
    mixed, new_state, last_rows = lax.map(one_sequence, (blocks, lengths, states))
    widened = last_rows.astype(jnp.float32)
    factor = lax.rsqrt(lax.optimization_barrier(jnp.mean(widened * widened, axis=1, keepdims=True)) + ROW_EPSILON)
    hidden = (widened * factor * final_gain).astype(jnp.bfloat16)
    logits = jnp.dot(hidden.astype(jnp.float32), vocab_table.T.astype(jnp.float32), preferred_element_type=jnp.float32)
    largest = lax.optimization_barrier(jnp.max(logits, axis=1))
    exp_total = lax.optimization_barrier(jnp.sum(jnp.exp(logits - largest[:, None]), axis=1))
    target = jnp.take_along_axis(logits, next_token[:, None], axis=1)[:, 0]
    log_likelihood = target - (largest + jnp.log(exp_total))
    return (mixed.reshape(tokens.shape), new_state, log_likelihood)
```

```python
import jax
import jax.numpy as jnp
from jax import lax
from jax.experimental import pallas as pl
from jax.experimental.pallas import tpu as pltpu
from jax.sharding import PartitionSpec as P

HEAD_DIM = 128
REFLECT = 3
NEW_POSITIONS = 128
CHUNK = 32
BASE = 8
STEPS = CHUNK * REFLECT
BLOCKS = 2 * REFLECT + 1

ROW_EPSILON = 1e-05
KEY_EPSILON = 1e-06


NN = (((1,), (0,)), ((), ()))
NT = (((1,), (1,)), ((), ()))
TN = (((0,), (0,)), ((), ()))


def halves(a):
    high = a.astype(jnp.bfloat16)
    return high, (a - high.astype(jnp.float32)).astype(jnp.bfloat16)


def dot1(a, b, dims=NN):
    return lax.dot_general(
        a.astype(jnp.bfloat16), b.astype(jnp.bfloat16), dims, preferred_element_type=jnp.float32
    )


def dot3(a, b, dims=NN):
    ah, al = halves(a)
    bh, bl = halves(b)
    cross = dot1(ah, bl, dims) + dot1(al, bh, dims)
    return dot1(ah, bh, dims) + cross


def silu(x):
    return x / (1.0 + jnp.exp(-x))


def interleave(parts):
    pieces = []
    for b in range(CHUNK // BASE):
        for part in parts:
            pieces.append(part[b * BASE : (b + 1) * BASE])
    return jnp.concatenate(pieces, axis=0)


def position_of(r):
    b = jnp.zeros_like(r)
    for n in range(1, CHUNK // BASE):
        b = b + (r >= n * BASE * REFLECT).astype(jnp.int32)
    rest = r - b * (BASE * REFLECT)
    j = jnp.zeros_like(r)
    for n in range(1, REFLECT):
        j = j + (rest >= n * BASE).astype(jnp.int32)
    return b * BASE + rest - j * BASE, j


def mixer_kernel(head_count, *refs):
    index_ref, lengths_ref, rate_ref = refs[:3]
    token_refs = refs[3 : 3 + head_count]
    (gain_ref, mix_ref, rate_weight_ref, head_gain_ref, state_ref) = refs[
        3 + head_count : 8 + head_count
    ]
    normed_ref, new_state_ref = refs[8 + head_count : 10 + head_count]
    scaled_ref, inverse_ref, rates_ref, projected_ref = refs[10 + head_count :]
    h = pl.program_id(0)
    width = token_refs[0].shape[1]
    sequences = state_ref.shape[0]

    @pl.when(h == 0)
    def _():
        squares = 0.0
        for k in range(head_count):
            at = pl.multiple_of((index_ref[0] ^ k) * width, width)
            wide = token_refs[k][...].astype(jnp.float32)
            squares = squares + jnp.sum(wide * wide, axis=1, keepdims=True)
            scaled_ref[:, pl.ds(at, width)] = (wide * gain_ref[:, pl.ds(at, width)]).astype(
                jnp.bfloat16
            )
        inverse = lax.rsqrt(squares / (width * head_count) + ROW_EPSILON)
        inverse_ref[...] = inverse
        rates_ref[...] = (
            jnp.dot(scaled_ref[...], rate_weight_ref[...], preferred_element_type=jnp.float32)
            * inverse
        )

    projected_ref[...] = (
        jnp.dot(scaled_ref[...], mix_ref[...], preferred_element_type=jnp.float32)
        * inverse_ref[...]
    )
    new_state_ref[...] = state_ref[...]
    decay_rate = rate_ref[h]

    def chunk_step(c, carry):
        square = (STEPS, STEPS)
        p_r, j_r = position_of(lax.broadcasted_iota(jnp.int32, square, 0))
        p_c, j_c = position_of(lax.broadcasted_iota(jnp.int32, square, 1))
        same = p_r == p_c
        eye = same & (j_r == j_c)
        strict = (p_r > p_c) | (same & (j_r > j_c))
        up_to = p_r <= p_c
        q_pos = lax.broadcasted_iota(jnp.int32, (CHUNK, STEPS), 0)
        q_col, q_j = position_of(lax.broadcasted_iota(jnp.int32, (CHUNK, STEPS), 1))
        visible = q_col <= q_pos
        q_pick = (q_col == q_pos) & (q_j == 0)
        identity = jnp.where(eye, 1.0, 0.0)
        each = range(sequences)
        starts = [pl.multiple_of(s * NEW_POSITIONS + c * CHUNK, CHUNK) for s in each]

        keys, lefts, values, betas, rows, cols, qcums, totals = [], [], [], [], [], [], [], []
        for s in each:
            at = pl.ds(starts[s], CHUNK)
            block = [
                silu(projected_ref[at, n * HEAD_DIM : (n + 1) * HEAD_DIM]) for n in range(BLOCKS)
            ]
            key_parts = [
                k * lax.rsqrt(jnp.sum(k * k, axis=1, keepdims=True) + KEY_EPSILON)
                for k in block[1 : REFLECT + 1]
            ]
            rates = rates_ref[at, :]
            lane = lax.broadcasted_iota(jnp.int32, rates.shape, 1)
            picked = [
                jnp.sum(
                    jnp.where(lane == h * (REFLECT + 1) + j, rates, 0.0), axis=1, keepdims=True
                )
                for j in range(REFLECT + 1)
            ]
            position = c * CHUNK + lax.broadcasted_iota(jnp.int32, (CHUNK, 1), 0)
            valid = position < lengths_ref[s]
            beta_parts = [
                jnp.where(valid, 2.0 / (1.0 + jnp.exp(-x)), 0.0) for x in picked[:REFLECT]
            ]
            d = picked[REFLECT]
            soft = jnp.maximum(d, 0.0) + jnp.log1p(jnp.exp(-jnp.abs(d)))
            log_decay = jnp.where(valid, -decay_rate * soft, 0.0)
            zero = jnp.zeros_like(log_decay)
            step_decay = interleave([log_decay] + [zero] * (REFLECT - 1))
            row = jnp.sum(jnp.where(up_to, step_decay, 0.0), axis=0, keepdims=True)
            key = interleave(key_parts)
            keys.append(key)
            lefts.append(jnp.concatenate([key, block[0]], axis=0))
            values.append(interleave(block[REFLECT + 1 :]))
            betas.append(interleave(beta_parts))
            rows.append(row)
            cols.append(jnp.sum(jnp.where(eye, row, 0.0), axis=1, keepdims=True))
            qcums.append(jnp.sum(jnp.where(q_pick, row, 0.0), axis=1, keepdims=True))
            totals.append(jnp.sum(log_decay, axis=0, keepdims=True))

        grams = [dot3(lefts[s], keys[s], NT) for s in each]
        lower = [
            betas[s]
            * jnp.exp(jnp.where(strict, cols[s] - rows[s], -jnp.inf))
            * grams[s][:STEPS]
            for s in each
        ]
        scores = [
            grams[s][STEPS:] * jnp.exp(jnp.where(visible, qcums[s] - rows[s], -jnp.inf))
            for s in each
        ]
        inner = [jnp.where(same, a, 0.0) for a in lower]
        inverses = [identity - d + dot1(d, d) for d in inner]
        level = 1
        while level < CHUNK:
            pair = ((p_r ^ p_c) < 2 * level) & ((p_r ^ p_c) >= level)
            off = [jnp.where(pair, a, 0.0) for a in lower]
            left = [dot1(inverses[s], off[s]) for s in each]
            inverses = [inverses[s] - dot1(left[s], inverses[s]) for s in each]
            level *= 2
        images = [dot3(lefts[s], new_state_ref[s, 0], NT) for s in each]
        sources = [
            betas[s] * (values[s] - jnp.exp(cols[s]) * images[s][:STEPS]) for s in each
        ]
        updates = [dot1(inverses[s], sources[s]) for s in each]
        residuals = [sources[s] - updates[s] - dot3(lower[s], updates[s]) for s in each]
        updates = [updates[s] + dot1(inverses[s], residuals[s]) for s in each]
        attended = [
            jnp.exp(qcums[s]) * images[s][STEPS:] + dot3(scores[s], updates[s]) for s in each
        ]
        for s in each:
            tail = jnp.exp(totals[s] - cols[s]) * keys[s]
            new_state_ref[s, 0] = jnp.exp(totals[s]) * new_state_ref[s, 0] + dot3(
                updates[s], tail, TN
            )
            o = attended[s]
            factor = lax.rsqrt(jnp.mean(o * o, axis=1, keepdims=True) + ROW_EPSILON)
            normed_ref[pl.ds(starts[s], CHUNK), :] = (o * factor * head_gain_ref[...]).astype(
                jnp.bfloat16
            )
        return carry

    lax.fori_loop(0, NEW_POSITIONS // CHUNK, chunk_step, 0)


def mixer(index, lengths, decay_rate, blocks, norm_gain, mix_weight, rate_weight, head_gain, states):
    rows, width = blocks[0].shape
    head_count = len(blocks)
    model_width = norm_gain.shape[0]
    sequences, local_heads = states.shape[:2]
    columns = BLOCKS * HEAD_DIM
    smem = pl.BlockSpec(memory_space=pltpu.SMEM)

    def whole(shape):
        return pl.BlockSpec(shape, lambda h: (0,) * len(shape))

    state_spec = pl.BlockSpec(
        (sequences, 1, HEAD_DIM, HEAD_DIM), lambda h: (0, h, 0, 0)
    )
    return pl.pallas_call(
        lambda *refs: mixer_kernel(head_count, *refs),
        grid=(local_heads,),
        in_specs=[smem, smem, smem]
        + [whole((rows, width))] * head_count
        + [
            whole((1, model_width)),
            pl.BlockSpec((model_width, columns), lambda h: (0, h)),
            whole(rate_weight.shape),
            whole((1, HEAD_DIM)),
            state_spec,
        ],
        out_specs=[pl.BlockSpec((rows, HEAD_DIM), lambda h: (0, h)), state_spec],
        out_shape=[
            jax.ShapeDtypeStruct((rows, local_heads * HEAD_DIM), jnp.bfloat16),
            jax.ShapeDtypeStruct(states.shape, jnp.float32),
        ],
        scratch_shapes=[
            pltpu.VMEM((rows, model_width), jnp.bfloat16),
            pltpu.VMEM((rows, 1), jnp.float32),
            pltpu.VMEM((rows, rate_weight.shape[1]), jnp.float32),
            pltpu.VMEM((rows, columns), jnp.float32),
        ],
        compiler_params=pltpu.CompilerParams(
            dimension_semantics=("arbitrary",), vmem_limit_bytes=48 * 1024 * 1024
        ),
        name="mixer",
    )(
        index,
        lengths,
        decay_rate,
        *blocks,
        norm_gain[None, :],
        mix_weight,
        rate_weight,
        head_gain[None, :],
        states,
    )


def project_kernel(head_count, *refs):
    lengths_ref = refs[0]
    normed_refs = refs[1 : 1 + head_count]
    weight_refs = refs[1 + head_count : 1 + 2 * head_count]
    tokens_ref, mixed_ref, last_ref, rounded_ref = refs[1 + 2 * head_count :]
    total = jnp.dot(normed_refs[0][...], weight_refs[0][...], preferred_element_type=jnp.float32)
    for k in range(1, head_count):
        total = total + jnp.dot(
            normed_refs[k][...], weight_refs[k][...], preferred_element_type=jnp.float32
        )
    mixed = (tokens_ref[...].astype(jnp.float32) + total).astype(jnp.bfloat16)
    mixed_ref[...] = mixed
    rounded_ref[...] = mixed.astype(jnp.float32)
    for s in range(last_ref.shape[0]):
        at = s * NEW_POSITIONS + lengths_ref[s] - 1
        last_ref[pl.ds(s, 1), :] = rounded_ref[pl.ds(at, 1), :]


def project(lengths, normed_blocks, weight_blocks, tokens):
    head_count = len(normed_blocks)
    vmem = pl.BlockSpec(memory_space=pltpu.VMEM)
    return pl.pallas_call(
        lambda *refs: project_kernel(head_count, *refs),
        in_specs=[pl.BlockSpec(memory_space=pltpu.SMEM)] + [vmem] * (2 * head_count + 1),
        out_specs=[vmem, vmem],
        out_shape=[
            jax.ShapeDtypeStruct(tokens.shape, jnp.bfloat16),
            jax.ShapeDtypeStruct((lengths.shape[0], tokens.shape[1]), jnp.float32),
        ],
        scratch_shapes=[pltpu.VMEM(tokens.shape, jnp.float32)],
        compiler_params=pltpu.CompilerParams(vmem_limit_bytes=48 * 1024 * 1024),
        name="project",
    )(lengths, *normed_blocks, *weight_blocks, tokens)


def swap(array, axis, k):
    size = lax.axis_size(axis)
    return lax.ppermute(array, axis, [(i, i ^ k) for i in range(size)])


def spread(array, axis):
    blocks = {0: array}
    bit = lax.axis_size(axis) // 2
    while bit >= 1:
        for k in list(blocks):
            blocks[k ^ bit] = swap(blocks[k], axis, bit)
        bit //= 2
    return [blocks[k] for k in range(len(blocks))]


def combine(parts):
    largest = jnp.max(parts[:, 0], axis=0)
    total = jnp.sum(parts[:, 1] * jnp.exp(parts[:, 0] - largest), axis=0)
    return jnp.stack([largest, total, jnp.sum(parts[:, 2], axis=0)])


def on_device(
    tokens,
    lengths,
    states,
    norm_gain,
    mix_weight,
    rate_weight,
    decay_rate,
    head_gain,
    out_weight,
    final_gain,
    vocab_table,
    next_token,
):
    sequences = lengths.shape[0]
    local_width = tokens.shape[1]
    model_width = norm_gain.shape[0]
    head_count = lax.axis_size("head")
    index = lax.axis_index("head")
    token_blocks = spread(tokens, "head")

    held = lax.optimization_barrier((out_weight, *token_blocks))
    early_weight, token_blocks = held[0], list(held[1:])
    weight_blocks = []
    for k in range(head_count):
        piece = lax.dynamic_slice(
            early_weight, (0, (index ^ k) * local_width), (out_weight.shape[0], local_width)
        )
        weight_blocks.append(swap(piece, "head", k) if k else piece)

    normed, new_state = mixer(
        index[None].astype(jnp.int32),
        lengths,
        decay_rate,
        token_blocks,
        norm_gain,
        mix_weight,
        rate_weight,
        head_gain,
        states,
    )
    mixed, last_rows = project(lengths, spread(normed, "head"), weight_blocks, tokens)
    last_rows = last_rows.astype(jnp.bfloat16)

    gathered = lax.all_gather(last_rows, "head", axis=1, tiled=True)
    everyone = lax.all_gather(gathered, "batch", axis=0, tiled=True)
    widened = everyone.astype(jnp.float32)
    factor = lax.rsqrt(jnp.mean(widened * widened, axis=1, keepdims=True) + ROW_EPSILON)
    hidden = (widened * factor * final_gain).astype(jnp.bfloat16)
    logits = jnp.dot(hidden, vocab_table.T, preferred_element_type=jnp.float32)
    vocab_here = vocab_table.shape[0]
    vocab_ids = lax.axis_index(("batch", "head")) * vocab_here + jnp.arange(vocab_here)
    largest = jnp.max(logits, axis=1)
    exp_total = jnp.sum(jnp.exp(logits - largest[:, None]), axis=1)
    target = jnp.sum(jnp.where(vocab_ids[None, :] == next_token[:, None], logits, 0.0), axis=1)
    stats = jnp.stack([largest, exp_total, target])
    stats = combine(lax.all_gather(stats, "head"))
    stats = combine(lax.all_gather(stats, "batch"))
    return (mixed, new_state, stats[2] - (stats[0] + jnp.log(stats[1])))


def solution(mesh):
    placed = (
        P("batch", "head"),
        P("batch"),
        P("batch", "head", None, None),
        P(),
        P(None, "head"),
        P(None, "head"),
        P("head"),
        P(),
        P("head", None),
        P(),
        P(("batch", "head"), None),
        P(),
    )
    return jax.shard_map(
        on_device,
        mesh=mesh,
        in_specs=placed,
        out_specs=(P("batch", "head"), P("batch", "head", None, None), P()),
        check_vma=False,
    )
```

```python
import jax
import jax.numpy as jnp
from jax import lax
from jax.experimental import pallas as pl
from jax.experimental.pallas import tpu as pltpu
from jax.sharding import PartitionSpec as P


HEAD_DIM = 128
REFLECT = 3
NEW_POSITIONS = 128
CHUNK = 32
BASE = 8
GROUP = 2
STEPS = CHUNK * REFLECT
BLOCKS = 2 * REFLECT + 1

ROW_EPSILON = 1e-05
KEY_EPSILON = 1e-06


NN = (((1,), (0,)), ((), ()))
NT = (((1,), (1,)), ((), ()))
TN = (((0,), (0,)), ((), ()))


def halves(a):
    high = a.astype(jnp.bfloat16)
    return high, (a - high.astype(jnp.float32)).astype(jnp.bfloat16)


def dot1(a, b, dims=NN):
    return lax.dot_general(
        a.astype(jnp.bfloat16), b.astype(jnp.bfloat16), dims, preferred_element_type=jnp.float32
    )


def dot3(a, b, dims=NN):
    ah, al = halves(a)
    bh, bl = halves(b)
    cross = dot1(ah, bl, dims) + dot1(al, bh, dims)
    return dot1(ah, bh, dims) + cross


def silu(x):
    return x / (1.0 + jnp.exp(-x))


def interleave(parts):
    pieces = []
    for b in range(CHUNK // BASE):
        for part in parts:
            pieces.append(part[b * BASE : (b + 1) * BASE])
    return jnp.concatenate(pieces, axis=0)


def position_of(r):
    b = jnp.zeros_like(r)
    for n in range(1, CHUNK // BASE):
        b = b + (r >= n * BASE * REFLECT).astype(jnp.int32)
    rest = r - b * (BASE * REFLECT)
    j = jnp.zeros_like(r)
    for n in range(1, REFLECT):
        j = j + (rest >= n * BASE).astype(jnp.int32)
    return b * BASE + rest - j * BASE, j


def mixer_kernel(head_count, *refs):
    index_ref, lengths_ref, rate_ref = refs[:3]
    token_refs = refs[3 : 3 + head_count]
    (gain_ref, mix_ref, rate_weight_ref, head_gain_ref, state_ref) = refs[
        3 + head_count : 8 + head_count
    ]
    normed_ref, new_state_ref = refs[8 + head_count : 10 + head_count]
    (scaled_ref, inverse_ref, rates_ref, projected_ref) = refs[10 + head_count : 14 + head_count]
    (fresh_ref, reads_ref, scores_ref, tails_ref, decays_ref) = refs[14 + head_count :]
    h = pl.program_id(0)
    width = token_refs[0].shape[1]
    sequences = state_ref.shape[0]

    @pl.when(h == 0)
    def _():
        squares = 0.0
        for k in range(head_count):
            at = pl.multiple_of((index_ref[0] ^ k) * width, width)
            wide = token_refs[k][...].astype(jnp.float32)
            squares = squares + jnp.sum(wide * wide, axis=1, keepdims=True)
            scaled_ref[:, pl.ds(at, width)] = (wide * gain_ref[:, pl.ds(at, width)]).astype(
                jnp.bfloat16
            )
        inverse = lax.rsqrt(squares / (width * head_count) + ROW_EPSILON)
        inverse_ref[...] = inverse
        rates_ref[...] = (
            jnp.dot(scaled_ref[...], rate_weight_ref[...], preferred_element_type=jnp.float32)
            * inverse
        )

    projected_ref[...] = (
        jnp.dot(scaled_ref[...], mix_ref[...], preferred_element_type=jnp.float32)
        * inverse_ref[...]
    )
    new_state_ref[...] = state_ref[...]
    decay_rate = rate_ref[h]

    def prepare(g, carry):
        square = (STEPS, STEPS)
        p_r, j_r = position_of(lax.broadcasted_iota(jnp.int32, square, 0))
        p_c, j_c = position_of(lax.broadcasted_iota(jnp.int32, square, 1))
        same = p_r == p_c
        eye = same & (j_r == j_c)
        strict = (p_r > p_c) | (same & (j_r > j_c))
        up_to = p_r <= p_c
        q_pos = lax.broadcasted_iota(jnp.int32, (CHUNK, STEPS), 0)
        q_col, q_j = position_of(lax.broadcasted_iota(jnp.int32, (CHUNK, STEPS), 1))
        visible = q_col <= q_pos
        q_pick = (q_col == q_pos) & (q_j == 0)
        identity = jnp.where(eye, 1.0, 0.0)
        chains = [(g * GROUP + n, s) for n in range(GROUP) for s in range(sequences)]
        each = range(len(chains))

        keys, lefts, values, betas, rows, cols, qcums, totals = [], [], [], [], [], [], [], []
        for c, s in chains:
            at = pl.ds(pl.multiple_of(s * NEW_POSITIONS + c * CHUNK, CHUNK), CHUNK)
            block = [
                silu(projected_ref[at, n * HEAD_DIM : (n + 1) * HEAD_DIM]) for n in range(BLOCKS)
            ]
            key_parts = [
                k * lax.rsqrt(jnp.sum(k * k, axis=1, keepdims=True) + KEY_EPSILON)
                for k in block[1 : REFLECT + 1]
            ]
            rates = rates_ref[at, :]
            lane = lax.broadcasted_iota(jnp.int32, rates.shape, 1)
            picked = [
                jnp.sum(
                    jnp.where(lane == h * (REFLECT + 1) + j, rates, 0.0), axis=1, keepdims=True
                )
                for j in range(REFLECT + 1)
            ]
            position = c * CHUNK + lax.broadcasted_iota(jnp.int32, (CHUNK, 1), 0)
            valid = position < lengths_ref[s]
            beta_parts = [
                jnp.where(valid, 2.0 / (1.0 + jnp.exp(-x)), 0.0) for x in picked[:REFLECT]
            ]
            d = picked[REFLECT]
            soft = jnp.maximum(d, 0.0) + jnp.log1p(jnp.exp(-jnp.abs(d)))
            log_decay = jnp.where(valid, -decay_rate * soft, 0.0)
            zero = jnp.zeros_like(log_decay)
            step_decay = interleave([log_decay] + [zero] * (REFLECT - 1))
            row = jnp.sum(jnp.where(up_to, step_decay, 0.0), axis=0, keepdims=True)
            key = interleave(key_parts)
            keys.append(key)
            lefts.append(jnp.concatenate([key, block[0]], axis=0))
            values.append(interleave(block[REFLECT + 1 :]))
            betas.append(interleave(beta_parts))
            rows.append(row)
            cols.append(jnp.sum(jnp.where(eye, row, 0.0), axis=1, keepdims=True))
            qcums.append(jnp.sum(jnp.where(q_pick, row, 0.0), axis=1, keepdims=True))
            totals.append(jnp.sum(log_decay, axis=0, keepdims=True))

        grams = [dot3(lefts[s], keys[s], NT) for s in each]
        lower = [
            betas[s]
            * jnp.exp(jnp.where(strict, cols[s] - rows[s], -jnp.inf))
            * grams[s][:STEPS]
            for s in each
        ]
        scores = [
            grams[s][STEPS:] * jnp.exp(jnp.where(visible, qcums[s] - rows[s], -jnp.inf))
            for s in each
        ]
        inner = [jnp.where(same, a, 0.0) for a in lower]
        inverses = [identity - d + dot1(d, d) for d in inner]
        level = 1
        while level < CHUNK:
            pair = ((p_r ^ p_c) < 2 * level) & ((p_r ^ p_c) >= level)
            off = [jnp.where(pair, a, 0.0) for a in lower]
            left = [dot1(inverses[s], off[s]) for s in each]
            inverses = [inverses[s] - dot1(left[s], inverses[s]) for s in each]
            level *= 2
        right = [
            jnp.concatenate([betas[n] * values[n], betas[n] * jnp.exp(cols[n]) * keys[n]], axis=1)
            for n in each
        ]
        solved = [dot1(inverses[n], right[n]) for n in each]
        residuals = [right[n] - solved[n] - dot3(lower[n], solved[n]) for n in each]
        solved = [solved[n] + dot1(inverses[n], residuals[n]) for n in each]
        for n in each:
            c, s = chains[n]
            slot = c * sequences + s
            fresh_ref[slot] = solved[n][:, :HEAD_DIM]
            reads_ref[slot, :STEPS] = solved[n][:, HEAD_DIM:]
            reads_ref[slot, STEPS:] = jnp.exp(qcums[n]) * lefts[n][STEPS:]
            scores_ref[slot] = scores[n]
            tails_ref[slot] = jnp.exp(totals[n] - cols[n]) * keys[n]
            decays_ref[slot] = jnp.broadcast_to(jnp.exp(totals[n]), (8, HEAD_DIM))
        return carry

    lax.fori_loop(0, NEW_POSITIONS // (CHUNK * GROUP), prepare, 0)

    def advance(c, carry):
        each = range(sequences)
        slots = [c * sequences + s for s in each]
        images = [dot3(reads_ref[slots[s]], new_state_ref[s, 0], NT) for s in each]
        updates = [fresh_ref[slots[s]] - images[s][:STEPS] for s in each]
        for s in each:
            new_state_ref[s, 0] = decays_ref[slots[s], 0:1, :] * new_state_ref[s, 0] + dot3(
                updates[s], tails_ref[slots[s]], TN
            )
        for s in each:
            o = images[s][STEPS:] + dot3(scores_ref[slots[s]], updates[s])
            factor = lax.rsqrt(jnp.mean(o * o, axis=1, keepdims=True) + ROW_EPSILON)
            at = pl.multiple_of(s * NEW_POSITIONS + c * CHUNK, CHUNK)
            normed_ref[pl.ds(at, CHUNK), :] = (o * factor * head_gain_ref[...]).astype(
                jnp.bfloat16
            )
        return carry

    lax.fori_loop(0, NEW_POSITIONS // CHUNK, advance, 0)


def mixer(index, lengths, decay_rate, blocks, norm_gain, mix_weight, rate_weight, head_gain, states):
    rows, width = blocks[0].shape
    head_count = len(blocks)
    model_width = norm_gain.shape[0]
    sequences, local_heads = states.shape[:2]
    columns = BLOCKS * HEAD_DIM
    slots = sequences * NEW_POSITIONS // CHUNK
    smem = pl.BlockSpec(memory_space=pltpu.SMEM)

    def whole(shape):
        return pl.BlockSpec(shape, lambda h: (0,) * len(shape))

    state_spec = pl.BlockSpec(
        (sequences, 1, HEAD_DIM, HEAD_DIM), lambda h: (0, h, 0, 0)
    )
    return pl.pallas_call(
        lambda *refs: mixer_kernel(head_count, *refs),
        grid=(local_heads,),
        in_specs=[smem, smem, smem]
        + [whole((rows, width))] * head_count
        + [
            whole((1, model_width)),
            pl.BlockSpec((model_width, columns), lambda h: (0, h)),
            whole(rate_weight.shape),
            whole((1, HEAD_DIM)),
            state_spec,
        ],
        out_specs=[pl.BlockSpec((rows, HEAD_DIM), lambda h: (0, h)), state_spec],
        out_shape=[
            jax.ShapeDtypeStruct((rows, local_heads * HEAD_DIM), jnp.bfloat16),
            jax.ShapeDtypeStruct(states.shape, jnp.float32),
        ],
        scratch_shapes=[
            pltpu.VMEM((rows, model_width), jnp.bfloat16),
            pltpu.VMEM((rows, 1), jnp.float32),
            pltpu.VMEM((rows, rate_weight.shape[1]), jnp.float32),
            pltpu.VMEM((rows, columns), jnp.float32),
            pltpu.VMEM((slots, STEPS, HEAD_DIM), jnp.float32),
            pltpu.VMEM((slots, STEPS + CHUNK, HEAD_DIM), jnp.float32),
            pltpu.VMEM((slots, CHUNK, STEPS), jnp.float32),
            pltpu.VMEM((slots, STEPS, HEAD_DIM), jnp.float32),
            pltpu.VMEM((slots, 8, HEAD_DIM), jnp.float32),
        ],
        cost_estimate=pl.CostEstimate(
            flops=24 * rows * model_width * columns,
            bytes_accessed=2 * model_width * columns * local_heads,
            transcendentals=0,
        ),
        compiler_params=pltpu.CompilerParams(
            dimension_semantics=("arbitrary",), vmem_limit_bytes=48 * 1024 * 1024
        ),
        name="mixer",
    )(
        index,
        lengths,
        decay_rate,
        *blocks,
        norm_gain[None, :],
        mix_weight,
        rate_weight,
        head_gain[None, :],
        states,
    )


def project_kernel(head_count, *refs):
    lengths_ref = refs[0]
    normed_refs = refs[1 : 1 + head_count]
    weight_refs = refs[1 + head_count : 1 + 2 * head_count]
    tokens_ref, mixed_ref, last_ref, rounded_ref = refs[1 + 2 * head_count :]
    total = jnp.dot(normed_refs[0][...], weight_refs[0][...], preferred_element_type=jnp.float32)
    for k in range(1, head_count):
        total = total + jnp.dot(
            normed_refs[k][...], weight_refs[k][...], preferred_element_type=jnp.float32
        )
    mixed = (tokens_ref[...].astype(jnp.float32) + total).astype(jnp.bfloat16)
    mixed_ref[...] = mixed
    rounded_ref[...] = mixed.astype(jnp.float32)
    for s in range(last_ref.shape[0]):
        at = s * NEW_POSITIONS + lengths_ref[s] - 1
        last_ref[pl.ds(s, 1), :] = rounded_ref[pl.ds(at, 1), :]


def project(lengths, normed_blocks, weight_blocks, tokens):
    head_count = len(normed_blocks)
    vmem = pl.BlockSpec(memory_space=pltpu.VMEM)
    return pl.pallas_call(
        lambda *refs: project_kernel(head_count, *refs),
        in_specs=[pl.BlockSpec(memory_space=pltpu.SMEM)] + [vmem] * (2 * head_count + 1),
        out_specs=[vmem, vmem],
        out_shape=[
            jax.ShapeDtypeStruct(tokens.shape, jnp.bfloat16),
            jax.ShapeDtypeStruct((lengths.shape[0], tokens.shape[1]), jnp.float32),
        ],
        scratch_shapes=[pltpu.VMEM(tokens.shape, jnp.float32)],
        compiler_params=pltpu.CompilerParams(vmem_limit_bytes=48 * 1024 * 1024),
        name="project",
    )(lengths, *normed_blocks, *weight_blocks, tokens)


def swap(array, axis, k):
    size = lax.axis_size(axis)
    return lax.ppermute(array, axis, [(i, i ^ k) for i in range(size)])


def spread(array, axis):
    blocks = {0: array}
    bit = lax.axis_size(axis) // 2
    while bit >= 1:
        for k in list(blocks):
            blocks[k ^ bit] = swap(blocks[k], axis, bit)
        bit //= 2
    return [blocks[k] for k in range(len(blocks))]


def score_kernel(batch_count, head_count, *refs):
    index_ref, next_ref, gain_ref, table_ref = refs[:4]
    row_refs = refs[4 : 4 + batch_count]
    stats_ref, everyone_ref = refs[4 + batch_count :]
    sequences, model_width = row_refs[0].shape
    width = model_width // head_count
    for m in range(batch_count):
        rows = row_refs[m][...].astype(jnp.float32)
        at = (index_ref[0] ^ m) * sequences
        for k in range(head_count):
            to = pl.multiple_of((index_ref[1] ^ k) * width, width)
            for r in range(sequences):
                everyone_ref[pl.ds(at + r, 1), pl.ds(to, width)] = rows[
                    r : r + 1, k * width : (k + 1) * width
                ]
    wide = everyone_ref[...]
    factor = lax.rsqrt(jnp.mean(wide * wide, axis=1, keepdims=True) + ROW_EPSILON)
    hidden = (wide * factor * gain_ref[...]).astype(jnp.bfloat16)
    logits = lax.dot_general(hidden, table_ref[...], NT, preferred_element_type=jnp.float32)
    ids = index_ref[2] + lax.broadcasted_iota(jnp.int32, logits.shape, 1)
    largest = jnp.max(logits, axis=1, keepdims=True)
    total = jnp.sum(jnp.exp(logits - largest), axis=1, keepdims=True)
    target = jnp.sum(jnp.where(ids == next_ref[...], logits, 0.0), axis=1, keepdims=True)
    lane = lax.broadcasted_iota(jnp.int32, stats_ref.shape, 1)
    stats_ref[...] = jnp.where(lane == 0, largest, jnp.where(lane == 1, total, target))


def score(index, next_token, final_gain, vocab_table, rows, head_count):
    everyone = (len(rows) * rows[0].shape[0], rows[0].shape[1])
    vmem = pl.BlockSpec(memory_space=pltpu.VMEM)
    return pl.pallas_call(
        lambda *refs: score_kernel(len(rows), head_count, *refs),
        in_specs=[pl.BlockSpec(memory_space=pltpu.SMEM)] + [vmem] * (3 + len(rows)),
        out_specs=vmem,
        out_shape=jax.ShapeDtypeStruct((everyone[0], HEAD_DIM), jnp.float32),
        scratch_shapes=[pltpu.VMEM(everyone, jnp.float32)],
        name="score",
    )(index, next_token[:, None], final_gain[None, :], vocab_table, *rows)


def combine_kernel(finish, index_ref, *refs):
    part_refs, out_ref, all_ref = refs[:-2], refs[-2], refs[-1]
    count = len(part_refs)
    for k in range(count):
        all_ref[index_ref[0] ^ k] = part_refs[k][...]
    parts = [all_ref[k] for k in range(count)]
    largest = parts[0][:, 0:1]
    for part in parts[1:]:
        largest = jnp.maximum(largest, part[:, 0:1])
    total, target = 0.0, 0.0
    for part in parts:
        total = total + part[:, 1:2] * jnp.exp(part[:, 0:1] - largest)
        target = target + part[:, 2:3]
    if finish:
        out_ref[...] = jnp.broadcast_to(target - (largest + jnp.log(total)), out_ref.shape)
    else:
        lane = lax.broadcasted_iota(jnp.int32, out_ref.shape, 1)
        out_ref[...] = jnp.where(lane == 0, largest, jnp.where(lane == 1, total, target))


def combine(index, parts, finish):
    vmem = pl.BlockSpec(memory_space=pltpu.VMEM)
    return pl.pallas_call(
        lambda *refs: combine_kernel(finish, *refs),
        in_specs=[pl.BlockSpec(memory_space=pltpu.SMEM)] + [vmem] * len(parts),
        out_specs=vmem,
        out_shape=jax.ShapeDtypeStruct(parts[0].shape, jnp.float32),
        scratch_shapes=[pltpu.VMEM((len(parts),) + parts[0].shape, jnp.float32)],
        name="combine",
    )(index, *parts)


def direct(array, axis):
    return [array] + [swap(array, axis, k) for k in range(1, lax.axis_size(axis))]


def on_device(
    tokens,
    lengths,
    states,
    norm_gain,
    mix_weight,
    rate_weight,
    decay_rate,
    head_gain,
    out_weight,
    final_gain,
    vocab_table,
    next_token,
):
    local_width = tokens.shape[1]
    head_count = lax.axis_size("head")
    index = lax.axis_index("head")
    token_blocks = spread(tokens, "head")

    held = lax.optimization_barrier((out_weight, *token_blocks))
    early_weight, token_blocks = held[0], list(held[1:])
    weight_blocks = []
    for k in range(head_count):
        piece = lax.dynamic_slice(
            early_weight, (0, (index ^ k) * local_width), (out_weight.shape[0], local_width)
        )
        weight_blocks.append(swap(piece, "head", k) if k else piece)

    normed, new_state = mixer(
        index[None].astype(jnp.int32),
        lengths,
        decay_rate,
        token_blocks,
        norm_gain,
        mix_weight,
        rate_weight,
        head_gain,
        states,
    )
    mixed, last_rows = project(lengths, spread(normed, "head"), weight_blocks, tokens)
    last_rows = last_rows.astype(jnp.bfloat16)

    batch_index = lax.axis_index("batch").astype(jnp.int32)
    head_index = index.astype(jnp.int32)
    vocab_start = (batch_index * head_count + head_index) * vocab_table.shape[0]
    joined = jnp.concatenate(direct(last_rows, "head"), axis=1)
    stats = score(
        jnp.stack([batch_index, head_index, vocab_start]),
        next_token,
        final_gain,
        vocab_table,
        direct(joined, "batch"),
        head_count,
    )
    stats = combine(head_index[None], direct(stats, "head"), False)
    scored = combine(batch_index[None], direct(stats, "batch"), True)
    return (mixed, new_state, scored[:, 0])


def solution(mesh):
    placed = (
        P("batch", "head"),
        P("batch"),
        P("batch", "head", None, None),
        P(),
        P(None, "head"),
        P(None, "head"),
        P("head"),
        P(),
        P("head", None),
        P(),
        P(("batch", "head"), None),
        P(),
    )
    return jax.shard_map(
        on_device,
        mesh=mesh,
        in_specs=placed,
        out_specs=(P("batch", "head"), P("batch", "head", None, None), P()),
        check_vma=False,
    )
```

```python
import jax
import jax.numpy as jnp
from jax import lax
from jax.experimental import pallas as pl
from jax.experimental.pallas import tpu as pltpu
from jax.sharding import PartitionSpec as P


HEAD_DIM = 128
REFLECT = 3
NEW_POSITIONS = 128
CHUNK = 32
BASE = 8
GROUP = 2
STEPS = CHUNK * REFLECT
BLOCKS = 2 * REFLECT + 1

ROW_EPSILON = 1e-05
KEY_EPSILON = 1e-06


NN = (((1,), (0,)), ((), ()))
NT = (((1,), (1,)), ((), ()))
TN = (((0,), (0,)), ((), ()))


def halves(a):
    high = a.astype(jnp.bfloat16)
    return high, (a - high.astype(jnp.float32)).astype(jnp.bfloat16)


def dot1(a, b, dims=NN):
    return lax.dot_general(
        a.astype(jnp.bfloat16), b.astype(jnp.bfloat16), dims, preferred_element_type=jnp.float32
    )


def dot3(a, b, dims=NN):
    ah, al = halves(a)
    bh, bl = halves(b)
    cross = dot1(ah, bl, dims) + dot1(al, bh, dims)
    return dot1(ah, bh, dims) + cross


def silu(x):
    return x / (1.0 + jnp.exp(-x))


def interleave(parts):
    pieces = []
    for b in range(CHUNK // BASE):
        for part in parts:
            pieces.append(part[b * BASE : (b + 1) * BASE])
    return jnp.concatenate(pieces, axis=0)


def position_of(r):
    b = jnp.zeros_like(r)
    for n in range(1, CHUNK // BASE):
        b = b + (r >= n * BASE * REFLECT).astype(jnp.int32)
    rest = r - b * (BASE * REFLECT)
    j = jnp.zeros_like(r)
    for n in range(1, REFLECT):
        j = j + (rest >= n * BASE).astype(jnp.int32)
    return b * BASE + rest - j * BASE, j


def mixer_kernel(head_count, *refs):
    index_ref, lengths_ref, rate_ref = refs[:3]
    token_refs = refs[3 : 3 + head_count]
    (gain_ref, mix_ref, rate_weight_ref, head_gain_ref, state_ref) = refs[
        3 + head_count : 8 + head_count
    ]
    normed_ref, new_state_ref = refs[8 + head_count : 10 + head_count]
    (scaled_ref, inverse_ref, rates_ref, projected_ref) = refs[10 + head_count : 14 + head_count]
    (fresh_ref, reads_ref, scores_ref, tails_ref, decays_ref) = refs[14 + head_count :]
    h = pl.program_id(0)
    width = token_refs[0].shape[1]
    sequences = state_ref.shape[0]

    @pl.when(h == 0)
    def _():
        squares = 0.0
        for k in range(head_count):
            at = pl.multiple_of((index_ref[0] ^ k) * width, width)
            wide = token_refs[k][...].astype(jnp.float32)
            squares = squares + jnp.sum(wide * wide, axis=1, keepdims=True)
            scaled_ref[:, pl.ds(at, width)] = (wide * gain_ref[:, pl.ds(at, width)]).astype(
                jnp.bfloat16
            )
        inverse = lax.rsqrt(squares / (width * head_count) + ROW_EPSILON)
        inverse_ref[...] = inverse
        rates_ref[...] = (
            jnp.dot(scaled_ref[...], rate_weight_ref[...], preferred_element_type=jnp.float32)
            * inverse
        )

    projected_ref[...] = (
        jnp.dot(scaled_ref[...], mix_ref[...], preferred_element_type=jnp.float32)
        * inverse_ref[...]
    )
    new_state_ref[...] = state_ref[...]
    decay_rate = rate_ref[h]

    def prepare(g, carry):
        square = (STEPS, STEPS)
        p_r, j_r = position_of(lax.broadcasted_iota(jnp.int32, square, 0))
        p_c, j_c = position_of(lax.broadcasted_iota(jnp.int32, square, 1))
        same = p_r == p_c
        eye = same & (j_r == j_c)
        strict = (p_r > p_c) | (same & (j_r > j_c))
        up_to = p_r <= p_c
        q_pos = lax.broadcasted_iota(jnp.int32, (CHUNK, STEPS), 0)
        q_col, q_j = position_of(lax.broadcasted_iota(jnp.int32, (CHUNK, STEPS), 1))
        visible = q_col <= q_pos
        q_pick = (q_col == q_pos) & (q_j == 0)
        identity = jnp.where(eye, 1.0, 0.0)
        chains = [(g * GROUP + n, s) for n in range(GROUP) for s in range(sequences)]
        each = range(len(chains))

        keys, lefts, values, betas, rows, cols, qcums, totals = [], [], [], [], [], [], [], []
        for c, s in chains:
            at = pl.ds(pl.multiple_of(s * NEW_POSITIONS + c * CHUNK, CHUNK), CHUNK)
            block = [
                silu(projected_ref[at, n * HEAD_DIM : (n + 1) * HEAD_DIM]) for n in range(BLOCKS)
            ]
            key_parts = [
                k * lax.rsqrt(jnp.sum(k * k, axis=1, keepdims=True) + KEY_EPSILON)
                for k in block[1 : REFLECT + 1]
            ]
            rates = rates_ref[at, :]
            lane = lax.broadcasted_iota(jnp.int32, rates.shape, 1)
            picked = [
                jnp.sum(
                    jnp.where(lane == h * (REFLECT + 1) + j, rates, 0.0), axis=1, keepdims=True
                )
                for j in range(REFLECT + 1)
            ]
            position = c * CHUNK + lax.broadcasted_iota(jnp.int32, (CHUNK, 1), 0)
            valid = position < lengths_ref[s]
            beta_parts = [
                jnp.where(valid, 2.0 / (1.0 + jnp.exp(-x)), 0.0) for x in picked[:REFLECT]
            ]
            d = picked[REFLECT]
            soft = jnp.maximum(d, 0.0) + jnp.log1p(jnp.exp(-jnp.abs(d)))
            log_decay = jnp.where(valid, -decay_rate * soft, 0.0)
            zero = jnp.zeros_like(log_decay)
            step_decay = interleave([log_decay] + [zero] * (REFLECT - 1))
            row = jnp.sum(jnp.where(up_to, step_decay, 0.0), axis=0, keepdims=True)
            key = interleave(key_parts)
            keys.append(key)
            lefts.append(jnp.concatenate([key, block[0]], axis=0))
            values.append(interleave(block[REFLECT + 1 :]))
            betas.append(interleave(beta_parts))
            rows.append(row)
            cols.append(jnp.sum(jnp.where(eye, row, 0.0), axis=1, keepdims=True))
            qcums.append(jnp.sum(jnp.where(q_pick, row, 0.0), axis=1, keepdims=True))
            totals.append(jnp.sum(log_decay, axis=0, keepdims=True))

        grams = [dot3(lefts[s], keys[s], NT) for s in each]
        lower = [
            betas[s]
            * jnp.exp(jnp.where(strict, cols[s] - rows[s], -jnp.inf))
            * grams[s][:STEPS]
            for s in each
        ]
        scores = [
            grams[s][STEPS:] * jnp.exp(jnp.where(visible, qcums[s] - rows[s], -jnp.inf))
            for s in each
        ]
        inner = [jnp.where(same, a, 0.0) for a in lower]
        inverses = [identity - d + dot1(d, d) for d in inner]
        level = 1
        while level < CHUNK:
            pair = ((p_r ^ p_c) < 2 * level) & ((p_r ^ p_c) >= level)
            off = [jnp.where(pair, a, 0.0) for a in lower]
            left = [dot1(inverses[s], off[s]) for s in each]
            inverses = [inverses[s] - dot1(left[s], inverses[s]) for s in each]
            level *= 2
        right = [
            jnp.concatenate([betas[n] * values[n], betas[n] * jnp.exp(cols[n]) * keys[n]], axis=1)
            for n in each
        ]
        solved = [dot1(inverses[n], right[n]) for n in each]
        residuals = [right[n] - solved[n] - dot3(lower[n], solved[n]) for n in each]
        solved = [solved[n] + dot1(inverses[n], residuals[n]) for n in each]
        for n in each:
            c, s = chains[n]
            slot = c * sequences + s
            fresh_ref[slot] = solved[n][:, :HEAD_DIM]
            reads_ref[slot, :STEPS] = solved[n][:, HEAD_DIM:]
            reads_ref[slot, STEPS:] = jnp.exp(qcums[n]) * lefts[n][STEPS:]
            scores_ref[slot] = scores[n]
            tails_ref[slot] = jnp.exp(totals[n] - cols[n]) * keys[n]
            decays_ref[slot] = jnp.broadcast_to(jnp.exp(totals[n]), (8, HEAD_DIM))
        return carry

    lax.fori_loop(0, NEW_POSITIONS // (CHUNK * GROUP), prepare, 0)

    def advance(c, carry):
        each = range(sequences)
        slots = [c * sequences + s for s in each]
        images = [dot3(reads_ref[slots[s]], new_state_ref[s, 0], NT) for s in each]
        updates = [fresh_ref[slots[s]] - images[s][:STEPS] for s in each]
        for s in each:
            new_state_ref[s, 0] = decays_ref[slots[s], 0:1, :] * new_state_ref[s, 0] + dot3(
                updates[s], tails_ref[slots[s]], TN
            )
        for s in each:
            o = images[s][STEPS:] + dot3(scores_ref[slots[s]], updates[s])
            factor = lax.rsqrt(jnp.mean(o * o, axis=1, keepdims=True) + ROW_EPSILON)
            at = pl.multiple_of(s * NEW_POSITIONS + c * CHUNK, CHUNK)
            normed_ref[pl.ds(at, CHUNK), :] = (o * factor * head_gain_ref[...]).astype(
                jnp.bfloat16
            )
        return carry

    lax.fori_loop(0, NEW_POSITIONS // CHUNK, advance, 0)


def mixer(index, lengths, decay_rate, blocks, norm_gain, mix_weight, rate_weight, head_gain, states):
    rows, width = blocks[0].shape
    head_count = len(blocks)
    model_width = norm_gain.shape[0]
    sequences, local_heads = states.shape[:2]
    columns = BLOCKS * HEAD_DIM
    slots = sequences * NEW_POSITIONS // CHUNK
    smem = pl.BlockSpec(memory_space=pltpu.SMEM)

    def whole(shape):
        return pl.BlockSpec(shape, lambda h: (0,) * len(shape))

    state_spec = pl.BlockSpec(
        (sequences, 1, HEAD_DIM, HEAD_DIM), lambda h: (0, h, 0, 0)
    )
    return pl.pallas_call(
        lambda *refs: mixer_kernel(head_count, *refs),
        grid=(local_heads,),
        in_specs=[smem, smem, smem]
        + [whole((rows, width))] * head_count
        + [
            whole((1, model_width)),
            pl.BlockSpec((model_width, columns), lambda h: (0, h)),
            whole(rate_weight.shape),
            whole((1, HEAD_DIM)),
            state_spec,
        ],
        out_specs=[pl.BlockSpec((rows, HEAD_DIM), lambda h: (0, h)), state_spec],
        out_shape=[
            jax.ShapeDtypeStruct((rows, local_heads * HEAD_DIM), jnp.bfloat16),
            jax.ShapeDtypeStruct(states.shape, jnp.float32),
        ],
        scratch_shapes=[
            pltpu.VMEM((rows, model_width), jnp.bfloat16),
            pltpu.VMEM((rows, 1), jnp.float32),
            pltpu.VMEM((rows, rate_weight.shape[1]), jnp.float32),
            pltpu.VMEM((rows, columns), jnp.float32),
            pltpu.VMEM((slots, STEPS, HEAD_DIM), jnp.float32),
            pltpu.VMEM((slots, STEPS + CHUNK, HEAD_DIM), jnp.float32),
            pltpu.VMEM((slots, CHUNK, STEPS), jnp.float32),
            pltpu.VMEM((slots, STEPS, HEAD_DIM), jnp.float32),
            pltpu.VMEM((slots, 8, HEAD_DIM), jnp.float32),
        ],
        cost_estimate=pl.CostEstimate(
            flops=24 * rows * model_width * columns,
            bytes_accessed=2 * model_width * columns * local_heads,
            transcendentals=0,
        ),
        compiler_params=pltpu.CompilerParams(
            dimension_semantics=("arbitrary",), vmem_limit_bytes=48 * 1024 * 1024
        ),
        name="mixer",
    )(
        index,
        lengths,
        decay_rate,
        *blocks,
        norm_gain[None, :],
        mix_weight,
        rate_weight,
        head_gain[None, :],
        states,
    )


def project_kernel(head_count, *refs):
    lengths_ref = refs[0]
    normed_refs = refs[1 : 1 + head_count]
    weight_refs = refs[1 + head_count : 1 + 2 * head_count]
    tokens_ref, mixed_ref, last_ref, rounded_ref = refs[1 + 2 * head_count :]
    total = jnp.dot(normed_refs[0][...], weight_refs[0][...], preferred_element_type=jnp.float32)
    for k in range(1, head_count):
        total = total + jnp.dot(
            normed_refs[k][...], weight_refs[k][...], preferred_element_type=jnp.float32
        )
    mixed = (tokens_ref[...].astype(jnp.float32) + total).astype(jnp.bfloat16)
    mixed_ref[...] = mixed
    rounded_ref[...] = mixed.astype(jnp.float32)
    for s in range(last_ref.shape[0]):
        at = s * NEW_POSITIONS + lengths_ref[s] - 1
        last_ref[pl.ds(s, 1), :] = rounded_ref[pl.ds(at, 1), :]


def project(lengths, normed_blocks, weight_blocks, tokens):
    head_count = len(normed_blocks)
    vmem = pl.BlockSpec(memory_space=pltpu.VMEM)
    return pl.pallas_call(
        lambda *refs: project_kernel(head_count, *refs),
        in_specs=[pl.BlockSpec(memory_space=pltpu.SMEM)] + [vmem] * (2 * head_count + 1),
        out_specs=[vmem, vmem],
        out_shape=[
            jax.ShapeDtypeStruct(tokens.shape, jnp.bfloat16),
            jax.ShapeDtypeStruct((lengths.shape[0], tokens.shape[1]), jnp.float32),
        ],
        scratch_shapes=[pltpu.VMEM(tokens.shape, jnp.float32)],
        compiler_params=pltpu.CompilerParams(vmem_limit_bytes=48 * 1024 * 1024),
        name="project",
    )(lengths, *normed_blocks, *weight_blocks, tokens)


def swap(array, axis, k):
    size = lax.axis_size(axis)
    return lax.ppermute(array, axis, [(i, i ^ k) for i in range(size)])


def spread(array, axis):
    blocks = {0: array}
    bit = lax.axis_size(axis) // 2
    while bit >= 1:
        for k in list(blocks):
            blocks[k ^ bit] = swap(blocks[k], axis, bit)
        bit //= 2
    return [blocks[k] for k in range(len(blocks))]


def score_kernel(batch_count, head_count, *refs):
    index_ref, next_ref, gain_ref, table_ref = refs[:4]
    row_refs = refs[4 : 4 + batch_count]
    stats_ref, placed_ref, everyone_ref = refs[4 + batch_count :]
    sequences, model_width = row_refs[0].shape
    width = model_width // head_count
    for m in range(batch_count):
        rows = row_refs[m][...].astype(jnp.float32)
        for k in range(head_count):
            placed_ref[index_ref[0] ^ m, index_ref[1] ^ k] = rows[:, k * width : (k + 1) * width]
    for m in range(batch_count):
        for k in range(head_count):
            everyone_ref[
                m * sequences : (m + 1) * sequences, k * width : (k + 1) * width
            ] = placed_ref[m, k]
    wide = everyone_ref[...]
    factor = lax.rsqrt(jnp.mean(wide * wide, axis=1, keepdims=True) + ROW_EPSILON)
    hidden = (wide * factor * gain_ref[...]).astype(jnp.bfloat16)
    logits = lax.dot_general(hidden, table_ref[...], NT, preferred_element_type=jnp.float32)
    ids = index_ref[2] + lax.broadcasted_iota(jnp.int32, logits.shape, 1)
    largest = jnp.max(logits, axis=1, keepdims=True)
    total = jnp.sum(jnp.exp(logits - largest), axis=1, keepdims=True)
    target = jnp.sum(jnp.where(ids == next_ref[...], logits, 0.0), axis=1, keepdims=True)
    lane = lax.broadcasted_iota(jnp.int32, stats_ref.shape, 1)
    stats_ref[...] = jnp.where(lane == 0, largest, jnp.where(lane == 1, total, target))


def score(index, next_token, final_gain, vocab_table, rows, head_count):
    everyone = (len(rows) * rows[0].shape[0], rows[0].shape[1])
    vmem = pl.BlockSpec(memory_space=pltpu.VMEM)
    return pl.pallas_call(
        lambda *refs: score_kernel(len(rows), head_count, *refs),
        in_specs=[pl.BlockSpec(memory_space=pltpu.SMEM)] + [vmem] * (3 + len(rows)),
        out_specs=vmem,
        out_shape=jax.ShapeDtypeStruct((everyone[0], HEAD_DIM), jnp.float32),
        scratch_shapes=[
            pltpu.VMEM(
                (len(rows), head_count, rows[0].shape[0], rows[0].shape[1] // head_count),
                jnp.float32,
            ),
            pltpu.VMEM(everyone, jnp.float32),
        ],
        name="score",
    )(index, next_token[:, None], final_gain[None, :], vocab_table, *rows)


def combine_kernel(finish, index_ref, *refs):
    part_refs, out_ref, all_ref = refs[:-2], refs[-2], refs[-1]
    count = len(part_refs)
    for k in range(count):
        all_ref[index_ref[0] ^ k] = part_refs[k][...]
    parts = [all_ref[k] for k in range(count)]
    largest = parts[0][:, 0:1]
    for part in parts[1:]:
        largest = jnp.maximum(largest, part[:, 0:1])
    total, target = 0.0, 0.0
    for part in parts:
        total = total + part[:, 1:2] * jnp.exp(part[:, 0:1] - largest)
        target = target + part[:, 2:3]
    if finish:
        out_ref[...] = jnp.broadcast_to(target - (largest + jnp.log(total)), out_ref.shape)
    else:
        lane = lax.broadcasted_iota(jnp.int32, out_ref.shape, 1)
        out_ref[...] = jnp.where(lane == 0, largest, jnp.where(lane == 1, total, target))


def combine(index, parts, finish):
    vmem = pl.BlockSpec(memory_space=pltpu.VMEM)
    return pl.pallas_call(
        lambda *refs: combine_kernel(finish, *refs),
        in_specs=[pl.BlockSpec(memory_space=pltpu.SMEM)] + [vmem] * len(parts),
        out_specs=vmem,
        out_shape=jax.ShapeDtypeStruct(parts[0].shape, jnp.float32),
        scratch_shapes=[pltpu.VMEM((len(parts),) + parts[0].shape, jnp.float32)],
        name="combine",
    )(index, *parts)


def direct(array, axis):
    return [array] + [swap(array, axis, k) for k in range(1, lax.axis_size(axis))]


def on_device(
    tokens,
    lengths,
    states,
    norm_gain,
    mix_weight,
    rate_weight,
    decay_rate,
    head_gain,
    out_weight,
    final_gain,
    vocab_table,
    next_token,
):
    local_width = tokens.shape[1]
    head_count = lax.axis_size("head")
    index = lax.axis_index("head")
    token_blocks = spread(tokens, "head")

    held = lax.optimization_barrier((out_weight, *token_blocks))
    early_weight, token_blocks = held[0], list(held[1:])
    weight_blocks = []
    for k in range(head_count):
        piece = lax.dynamic_slice(
            early_weight, (0, (index ^ k) * local_width), (out_weight.shape[0], local_width)
        )
        weight_blocks.append(swap(piece, "head", k) if k else piece)

    normed, new_state = mixer(
        index[None].astype(jnp.int32),
        lengths,
        decay_rate,
        token_blocks,
        norm_gain,
        mix_weight,
        rate_weight,
        head_gain,
        states,
    )
    mixed, last_rows = project(lengths, spread(normed, "head"), weight_blocks, tokens)
    last_rows = last_rows.astype(jnp.bfloat16)

    batch_index = lax.axis_index("batch").astype(jnp.int32)
    head_index = index.astype(jnp.int32)
    vocab_start = (batch_index * head_count + head_index) * vocab_table.shape[0]
    joined = jnp.concatenate(direct(last_rows, "head"), axis=1)
    stats = score(
        jnp.stack([batch_index, head_index, vocab_start]),
        next_token,
        final_gain,
        vocab_table,
        direct(joined, "batch"),
        head_count,
    )
    stats = combine(head_index[None], direct(stats, "head"), False)
    scored = combine(batch_index[None], direct(stats, "batch"), True)
    return (mixed, new_state, scored[:, 0])


def solution(mesh):
    placed = (
        P("batch", "head"),
        P("batch"),
        P("batch", "head", None, None),
        P(),
        P(None, "head"),
        P(None, "head"),
        P("head"),
        P(),
        P("head", None),
        P(),
        P(("batch", "head"), None),
        P(),
    )
    return jax.shard_map(
        on_device,
        mesh=mesh,
        in_specs=placed,
        out_specs=(P("batch", "head"), P("batch", "head", None, None), P()),
        check_vma=False,
    )
```
